16 devices in a mesh: tp: 4 (over z, y), dp: 4 (over x, core).
Axes of the slice: x: 2, y: 2, z: 2, core: 2. Of those that a mesh axis runs over, the one named last changes fastest.
Arguments:
- hidden_in: bfloat16 [16384, 1280], P('dp')
- targets: bfloat16 [16384, 1280], P('dp')
- w_up: bfloat16 [4, 1280, 5120], P(None, None, 'tp')
- w_down: bfloat16 [4, 5120, 1280], P(None, 'tp')
Outputs:
- output 1: float32 [4, 1280, 5120], P(None, None, 'tp')
- output 2: float32 [4, 5120, 1280], P(None, 'tp')
All inputs are finite; a program needn't handle non-finite values.
Results may differ from the reference program's by a relative error of at most 0.0101971.
Values are sent between devices in bfloat16 or wider.
A program may use at most 1 GiB of HBM per device.

```python
import math
import jax
import jax.numpy as jnp
from jax import lax

D = 1280
FF = 5120
TOKENS = 16384
BLOCK_ROWS = 512
LAYERS = 4


def setup_inputs(seed: int = 0) -> dict:
    keys = jax.random.split(jax.random.key(seed), 4)
    tgt_scale = 2.0 * math.sqrt(TOKENS)
    hidden_in = jax.random.normal(keys[0], (TOKENS, D), jnp.float32)
    targets = tgt_scale * jax.random.normal(keys[1], (TOKENS, D), jnp.float32)
    w_up = jax.random.normal(keys[2], (LAYERS, D, FF), jnp.float32) * (D ** -0.5)
    w_down = jax.random.normal(keys[3], (LAYERS, FF, D), jnp.float32) * (FF ** -0.5)
    return {"hidden_in": hidden_in.astype(jnp.bfloat16), "targets": targets.astype(jnp.bfloat16), "w_up": w_up.astype(jnp.bfloat16), "w_down": w_down.astype(jnp.bfloat16)}


def gelu_tanh(value):
    return jax.nn.gelu(value, approximate=True)


def block_grads(hidden, target, w_up, w_down):
    def fwd_layer(h_cur, weights):
        up_w, down_w = weights
        pre_act = jnp.dot(h_cur, up_w, preferred_element_type=jnp.float32).astype(jnp.bfloat16)
        act_val = gelu_tanh(pre_act.astype(jnp.float32)).astype(jnp.bfloat16)
        branch = jnp.dot(act_val, down_w, preferred_element_type=jnp.float32).astype(jnp.bfloat16)
        return h_cur + branch, (h_cur, pre_act, act_val)

    h_last, saved = lax.scan(fwd_layer, hidden, (w_up, w_down))
    err_f32 = (h_last.astype(jnp.float32) - target.astype(jnp.float32)) / TOKENS

    def bwd_layer(g_cur, layer_in):
        h_in, pre_act, act_val, up_w, down_w = layer_in
        g_down = jnp.dot(act_val.T, g_cur, preferred_element_type=jnp.float32)
        d_act = jnp.dot(g_cur, down_w.T, preferred_element_type=jnp.float32)
        _, gelu_vjp = jax.vjp(gelu_tanh, pre_act.astype(jnp.float32))
        d_pre = gelu_vjp(d_act)[0].astype(jnp.bfloat16)
        g_up = jnp.dot(h_in.T, d_pre, preferred_element_type=jnp.float32)
        back_sum = g_cur.astype(jnp.float32) + jnp.dot(d_pre, up_w.T, preferred_element_type=jnp.float32)
        return back_sum.astype(jnp.bfloat16), (g_up, g_down)

    _, grads = lax.scan(bwd_layer, err_f32.astype(jnp.bfloat16), (saved[0], saved[1], saved[2], w_up, w_down), reverse=True)
    return grads


def reference(hidden_in, targets, w_up, w_down):
    num_blocks = TOKENS // BLOCK_ROWS
    hid_blocks = hidden_in.reshape(num_blocks, BLOCK_ROWS, D)
    tgt_blocks = targets.reshape(num_blocks, BLOCK_ROWS, D)

    def accumulate(acc_grads, block_pair):
        g_up, g_down = block_grads(block_pair[0], block_pair[1], w_up, w_down)
        return (acc_grads[0] + g_up, acc_grads[1] + g_down), None

    zero_grads = (jnp.zeros((LAYERS, D, FF), jnp.float32), jnp.zeros((LAYERS, FF, D), jnp.float32))
    (grad_up, grad_down), _ = lax.scan(accumulate, zero_grads, (hid_blocks, tgt_blocks))
    return grad_up, grad_down
```

```python
import jax
import jax.numpy as jnp
from jax import lax
from jax.sharding import PartitionSpec as P


F32, BF16 = jnp.float32, jnp.bfloat16
X_SWAP = [(0, 2), (1, 3), (2, 0), (3, 1)]
C_SWAP = [(0, 1), (1, 0), (2, 3), (3, 2)]
NT = (((1,), (1,)), ((), ()))
TN = (((0,), (0,)), ((), ()))


def dot(a, b, dims=(((1,), (0,)), ((), ()))):
    return lax.dot_general(a, b, dims, preferred_element_type=F32)


def gelu(value):
    return jax.nn.gelu(value, approximate=True)


def gelu_bwd(pre, d_act):
    _, vjp = jax.vjp(gelu, pre.astype(F32))
    return vjp(d_act)[0].astype(BF16)


def x_swap(value):
    return lax.ppermute(value, "dp", X_SWAP)


def c_swap(value):
    return lax.ppermute(value, "dp", C_SWAP)


def gather_tokens(value):
    pair = jnp.concatenate([value, x_swap(value)], axis=0)
    return jnp.concatenate([pair, c_swap(pair)], axis=0)


def local_step(hidden, targets, w_up, w_down, total_tokens):
    layers, dim, cols = w_up.shape
    tp = lax.axis_size("tp")
    rows = hidden.shape[0] // tp
    tp_i, dp_i = lax.axis_index("tp"), lax.axis_index("dp")
    x_i, c_i = dp_i // 2, dp_i % 2
    half, quarter = cols // 2, cols // 4
    h_cur = lax.dynamic_slice_in_dim(hidden, tp_i * rows, rows, 0)
    t_cur = lax.dynamic_slice_in_dim(targets, tp_i * rows, rows, 0)

    def mine(full):
        blocks = full.reshape(tp, 2, quarter, dim)
        return lax.dynamic_index_in_dim(blocks, x_i, 1, keepdims=False).reshape(tp * quarter, dim)

    ups, downs = [], []
    for layer in range(layers):
        up_part = lax.dynamic_slice_in_dim(w_up[layer], c_i * half, half, 1).T
        down_part = lax.dynamic_slice_in_dim(w_down[layer], c_i * half, half, 0)
        up_own = lax.all_gather(up_part, "tp", axis=0, tiled=True)
        down_own = lax.all_gather(down_part, "tp", axis=0, tiled=True)
        ups.append((up_own, c_swap(up_own)))
        downs.append((down_own, c_swap(down_own)))

    saved = []
    for layer in range(layers):
        pres = [dot(h_cur, w, NT).astype(BF16) for w in ups[layer]]
        acts = [gelu(p.astype(F32)).astype(BF16) for p in pres]
        branch = (dot(acts[0], downs[layer][0]) + dot(acts[1], downs[layer][1])).astype(BF16)
        h_all = gather_tokens(h_cur)
        pre_q = dot(h_all, mine(ups[layer][0]), NT).astype(BF16)
        saved.append((pres, h_all, pre_q))
        h_cur = h_cur + branch

    g_cur = ((h_cur.astype(F32) - t_cur.astype(F32)) / total_tokens).astype(BF16)
    out_up = jnp.zeros((layers, dim, cols), F32)
    out_down = jnp.zeros((layers, cols, dim), F32)

    def finish(grad_q, flip):
        part = lax.psum_scatter(grad_q, "tp", scatter_dimension=0, tiled=True)
        other = x_swap(part)
        both = jnp.where(x_i == 0, jnp.concatenate([part, other], 0), jnp.concatenate([other, part], 0))
        both = both.T if flip else both
        return both, c_swap(both)

    for layer in reversed(range(layers)):
        pres, h_all, pre_q = saved[layer]
        g_all = gather_tokens(g_cur)
        if layer > 0:
            d_pres = [gelu_bwd(p, dot(g_cur, w, NT)) for p, w in zip(pres, downs[layer])]
            back = dot(d_pres[0], ups[layer][0]) + dot(d_pres[1], ups[layer][1])
            g_cur = (g_cur.astype(F32) + back).astype(BF16)
        act_q = gelu(pre_q.astype(F32)).astype(BF16)
        own, peer = finish(dot(act_q, g_all, TN), False)
        out_down = lax.dynamic_update_slice(out_down, own[None], (layer, c_i * half, 0))
        out_down = lax.dynamic_update_slice(out_down, peer[None], (layer, (1 - c_i) * half, 0))
        d_pre_q = gelu_bwd(pre_q, dot(g_all, mine(downs[layer][0]), NT))
        own, peer = finish(dot(d_pre_q, h_all, TN), True)
        out_up = lax.dynamic_update_slice(out_up, own[None], (layer, 0, c_i * half))
        out_up = lax.dynamic_update_slice(out_up, peer[None], (layer, 0, (1 - c_i) * half))
    return out_up, out_down


def solution(mesh):
    def grad_step(hidden_in, targets, w_up, w_down):
        def step(*args):
            return local_step(*args, total_tokens=hidden_in.shape[0])

        mapped = jax.shard_map(step, mesh=mesh, in_specs=(P("dp", None), P("dp", None), P(None, None, "tp"), P(None, "tp", None)), out_specs=(P(None, None, "tp"), P(None, "tp", None)), check_vma=False)
        return mapped(hidden_in, targets, w_up, w_down)

    return grad_step
```

```python
import jax
import jax.numpy as jnp
from jax import lax
from jax.sharding import PartitionSpec as P


F32, BF16 = jnp.float32, jnp.bfloat16
X_SWAP = [(0, 2), (1, 3), (2, 0), (3, 1)]
C_SWAP = [(0, 1), (1, 0), (2, 3), (3, 2)]
NT = (((1,), (1,)), ((), ()))
TN = (((0,), (0,)), ((), ()))


def dot(a, b, dims=(((1,), (0,)), ((), ()))):
    return lax.dot_general(a, b, dims, preferred_element_type=F32)


def gelu(value):
    return jax.nn.gelu(value, approximate=True)


def gelu_bwd(pre, d_act):
    _, vjp = jax.vjp(gelu, pre.astype(F32))
    return vjp(d_act)[0].astype(BF16)


def x_swap(value):
    return lax.ppermute(value, "dp", X_SWAP)


def c_swap(value):
    return lax.ppermute(value, "dp", C_SWAP)


def tie(*values):
    return lax.optimization_barrier(values)


def gather_tokens(value, other):
    pair = jnp.concatenate([value, other], axis=0)
    return jnp.concatenate([pair, c_swap(pair)], axis=0)


def local_step(hidden, targets, w_up, w_down, total_tokens):
    layers, dim, cols = w_up.shape
    last = layers - 1
    tp = lax.axis_size("tp")
    rows = hidden.shape[0] // tp
    tp_i, dp_i = lax.axis_index("tp"), lax.axis_index("dp")
    x_i, c_i = dp_i // 2, dp_i % 2
    half, quarter = cols // 2, cols // 4
    h_cur = lax.dynamic_slice_in_dim(hidden, tp_i * rows, rows, 0)
    t_cur = lax.dynamic_slice_in_dim(targets, tp_i * rows, rows, 0)

    def mine(full):
        blocks = full.reshape(tp, 2, quarter, dim)
        return lax.dynamic_index_in_dim(blocks, x_i, 1, keepdims=False).reshape(tp * quarter, dim)

    def up_part(layer):
        return jnp.where(c_i == 0, w_up[layer, :, :half], w_up[layer, :, half:]).T

    def down_part(layer):
        return lax.dynamic_slice_in_dim(w_down[layer], c_i * half, half, 0)

    parts = [up_part(0)[None]]
    parts += [jnp.stack([down_part(layer), up_part(layer + 1)]) for layer in range(last)]
    parts.append(down_part(last)[None])
    gathered = []
    for part in parts:
        gathered.append(lax.all_gather(part, "tp", axis=1, tiled=True))

    def quarter_forward(layer):
        pre = dot(saved[layer][1], mine(ups[layer][0]), NT).astype(BF16)
        act, vjp = jax.vjp(gelu, pre.astype(F32))
        return act.astype(BF16), vjp(jnp.ones_like(act))[0], mine(downs[layer][0])

    saved, ups, downs, quarters = [], [], [], []
    for layer in range(layers):
        if layer == 0:
            own, h_cur = tie(gathered[0], h_cur)
            ups.append((own[0], c_swap(own)[0]))
        h_x = x_swap(h_cur)
        h_all = gather_tokens(h_cur, h_x)
        pres = [dot(h_cur, w, NT).astype(BF16) for w in ups[layer]]
        acts = [gelu(p.astype(F32)).astype(BF16) for p in pres]
        done = quarter_forward(layer - 1) if layer > 0 else ()
        own, acts[0], acts[1], *done = tie(gathered[layer + 1], acts[0], acts[1], *done)
        if layer > 0:
            quarters.append(done)
        peer = c_swap(own)
        downs.append((own[0], peer[0]))
        if layer < last:
            ups.append((own[1], peer[1]))
        branch = (dot(acts[0], downs[layer][0]) + dot(acts[1], downs[layer][1])).astype(BF16)
        saved.append((pres, h_all))
        h_cur = h_cur + branch

    g_cur = ((h_cur.astype(F32) - t_cur.astype(F32)) / total_tokens).astype(BF16)
    g_x = x_swap(g_cur)
    quarters.append(list(quarter_forward(last)))

    def reduced(grad_q):
        return lax.psum_scatter(grad_q, "tp", scatter_dimension=0, tiled=True)

    red_up, red_down = [None] * layers, [None] * layers
    g_all = None
    for layer in reversed(range(layers)):
        pres, h_all = saved[layer]
        act_q, slope_q, down_q = quarters[layer]
        if layer > 0:
            d_acts = [dot(g_cur, w, NT) for w in downs[layer]]
            d_pres = [gelu_bwd(p, d) for p, d in zip(pres, d_acts)]
            if layer == last:
                g_x, act_q, d_pres[0], d_pres[1] = tie(g_x, act_q, d_pres[0], d_pres[1])
                g_all = gather_tokens(g_cur, g_x)
            back = dot(d_pres[0], ups[layer][0]) + dot(d_pres[1], ups[layer][1])
            g_next = (g_cur.astype(F32) + back).astype(BF16)
            g_x = x_swap(g_next)
            g_all, g_main = tie(g_all, g_next)
        grad_down = dot(act_q, g_all, TN)
        grad_down, g_all = tie(grad_down, g_all)
        red_down[layer] = reduced(grad_down)
        d_act_q = dot(g_all, down_q, NT)
        d_pre_q = (d_act_q * slope_q).astype(BF16)
        if layer > 0:
            g_x, d_pre_q = tie(g_x, d_pre_q)
            g_all = gather_tokens(g_next, g_x)
        grad_up = dot(d_pre_q, h_all, TN)
        if layer > 0:
            grad_up, g_cur = tie(grad_up, g_main)
        red_up[layer] = reduced(grad_up)

    def finish(part, flip):
        other = x_swap(part)
        both = jnp.where(x_i == 0, jnp.concatenate([part, other], 0), jnp.concatenate([other, part], 0))
        both = both.T if flip else both
        return both, c_swap(both)

    out_up = jnp.zeros((layers, dim, cols), F32)
    out_down = jnp.zeros((layers, cols, dim), F32)
    for layer in reversed(range(layers)):
        own, peer = finish(red_down[layer], False)
        out_down = lax.dynamic_update_slice(out_down, own[None], (layer, c_i * half, 0))
        out_down = lax.dynamic_update_slice(out_down, peer[None], (layer, (1 - c_i) * half, 0))
        own, peer = finish(red_up[layer], True)
        out_up = lax.dynamic_update_slice(out_up, own[None], (layer, 0, c_i * half))
        out_up = lax.dynamic_update_slice(out_up, peer[None], (layer, 0, (1 - c_i) * half))
    return out_up, out_down


def solution(mesh):
    def grad_step(hidden_in, targets, w_up, w_down):
        def step(*args):
            return local_step(*args, total_tokens=hidden_in.shape[0])

        mapped = jax.shard_map(step, mesh=mesh, in_specs=(P("dp", None), P("dp", None), P(None, None, "tp"), P(None, "tp", None)), out_specs=(P(None, None, "tp"), P(None, "tp", None)), check_vma=False)
        return mapped(hidden_in, targets, w_up, w_down)

    return grad_step
```
